256 devices in a mesh: outer: 32 (over z, y), inner: 8 (over x, core).
Axes of the slice: x: 4, y: 4, z: 8, core: 2. Of those that a mesh axis runs over, the one named last changes fastest.
Arguments:
- w_one: float32 [32, 8, 4, 128, 512], P('outer', 'inner')
- w_two: float32 [32, 8, 4, 512, 128], P('outer', 'inner')
- inputs: bfloat16 [32, 8, 16, 64, 128], P('outer', 'inner')
- targets: bfloat16 [32, 8, 16, 64, 128], P('outer', 'inner')
- mix_self: float32 [32, 8, 16], P('outer', 'inner')
Outputs:
- output 1: float32 [32, 8, 4, 128, 512], P('outer', 'inner')
- output 2: float32 [32, 8, 4, 512, 128], P('outer', 'inner')
All inputs are finite; a program needn't handle non-finite values.
Results may differ from the reference program's by a relative error of at most 0.00351111.
Values are sent between devices in bfloat16 or wider.
A program may use at most 768 MiB of HBM per device.

```python
import math
import jax
import jax.numpy as jnp
from jax import lax

OUTER_N = 32
INNER_N = 8
LAYERS = 4
STEPS = 16
BATCH = 64
D = 128
FF = 512

N_REPLICAS = OUTER_N * INNER_N
LOG_REPLICAS = N_REPLICAS.bit_length() - 1
LEARN_RATE = 1.5 / LAYERS
RMS_EPS = 1e-6
SPREAD = 0.6
TARGET_SCALE = 3.0


def setup_inputs(seed: int = 0) -> dict:
    sub_keys = jax.random.split(jax.random.key(seed), 7)
    spread_norm = 1.0 / math.sqrt(1.0 + SPREAD * SPREAD)
    base_one = jax.random.normal(sub_keys[0], (LAYERS, D, FF), jnp.float32)
    dev_one = jax.random.normal(sub_keys[1], (OUTER_N, INNER_N, LAYERS, D, FF), jnp.float32)
    w_one = (base_one + SPREAD * dev_one) * (spread_norm * D ** -0.5)
    base_two = jax.random.normal(sub_keys[2], (LAYERS, FF, D), jnp.float32)
    dev_two = jax.random.normal(sub_keys[3], (OUTER_N, INNER_N, LAYERS, FF, D), jnp.float32)
    w_two = (base_two + SPREAD * dev_two) * (spread_norm * FF ** -0.5)
    inputs = jax.random.normal(sub_keys[4], (OUTER_N, INNER_N, STEPS, BATCH, D), jnp.float32).astype(jnp.bfloat16)
    targets = (TARGET_SCALE * jax.random.normal(sub_keys[5], (OUTER_N, INNER_N, STEPS, BATCH, D), jnp.float32)).astype(jnp.bfloat16)
    mix_self = jax.random.uniform(sub_keys[6], (OUTER_N, INNER_N, STEPS), jnp.float32, 0.3, 0.7)
    return {'w_one': w_one, 'w_two': w_two, 'inputs': inputs, 'targets': targets, 'mix_self': mix_self}


def replica_loss(w_one, w_two, inputs, targets):
    def layer_body(hidden, weights):
        w_in, w_out = weights
        hid_f = hidden.astype(jnp.float32)
        normed = (hid_f * lax.rsqrt(jnp.mean(hid_f * hid_f, axis=-1, keepdims=True) + RMS_EPS)).astype(jnp.bfloat16)
        pre_act = jnp.dot(normed, w_in.astype(jnp.bfloat16), preferred_element_type=jnp.float32)
        act_bf = jax.nn.gelu(pre_act).astype(jnp.bfloat16)
        out_add = jnp.dot(act_bf, w_out.astype(jnp.bfloat16), preferred_element_type=jnp.float32)
        return (hid_f + out_add).astype(jnp.bfloat16), None
    final_hidden = lax.scan(layer_body, inputs, (w_one, w_two))[0]
    err_val = final_hidden.astype(jnp.float32) - targets.astype(jnp.float32)
    return jnp.mean(err_val * err_val)


def reference(w_one, w_two, inputs, targets, mix_self):
    flat_one = w_one.reshape((N_REPLICAS, LAYERS, D, FF))
    flat_two = w_two.reshape((N_REPLICAS, LAYERS, FF, D))
    flat_in = inputs.reshape((N_REPLICAS, STEPS, BATCH, D))
    flat_tgt = targets.reshape((N_REPLICAS, STEPS, BATCH, D))
    flat_mix = mix_self.reshape((N_REPLICAS, STEPS))
    grad_fn = jax.grad(replica_loss, argnums=(0, 1))

    def one_grad(packed):
        return grad_fn(packed[0], packed[1], packed[2], packed[3])

    for step_idx in range(STEPS):
        grad_one, grad_two = lax.map(one_grad, (flat_one, flat_two, flat_in[:, step_idx], flat_tgt[:, step_idx]))
        peer_shift = 2 ** (step_idx % LOG_REPLICAS)
        peer_one = jnp.roll(flat_one.astype(jnp.bfloat16), peer_shift, axis=0).astype(jnp.float32)
        peer_two = jnp.roll(flat_two.astype(jnp.bfloat16), peer_shift, axis=0).astype(jnp.float32)
        self_weight = flat_mix[:, step_idx][:, None, None, None]
        flat_one = self_weight * flat_one + (1.0 - self_weight) * peer_one - LEARN_RATE * grad_one
        flat_two = self_weight * flat_two + (1.0 - self_weight) * peer_two - LEARN_RATE * grad_two
    return flat_one.reshape(w_one.shape), flat_two.reshape(w_two.shape)
```

```python
import jax
import jax.numpy as jnp
from jax import lax
from jax.experimental import pallas as pl
from jax.experimental.pallas import tpu as pltpu
from jax.sharding import PartitionSpec as P

RMS_EPS = 1e-6
RATE_BASE = 1.5
MESH = pl.DeviceIdType.MESH
GELU_A = 0.7978845608028654
GELU_B = 0.7978845608028654 * 0.044715


def two_power(k):
    return (1 + k % 2) * (1 + 3 * ((k // 2) % 2)) * (1 + 15 * (k // 4))


def run_kernel(n_dev, n_inner, mix_ref, a_hbm, t_hbm, w1_hbm, w2_hbm, o1_hbm, o2_hbm,
               a_ref, t_ref, w1, w2, q1, q2, r1, r2, xs, us, gs, hs, invs,
               io_sem, send_sem, recv_sem):
    n_steps, rows, feat = a_ref.shape
    n_layers = w1.shape[0]
    log_g = n_dev.bit_length() - 1
    rate = RATE_BASE / n_layers
    me = lax.axis_index('outer') * n_inner + lax.axis_index('inner')
    n_chunks = 2 * n_layers

    def as_id(r):
        return (r // n_inner, r % n_inner)

    def load_in(c):
        l, m = c // 2, c % 2
        src, dst = (w1_hbm, w1) if m == 0 else (w2_hbm, w2)
        return pltpu.make_async_copy(src.at[l], dst.at[l], io_sem.at[c])

    def load_out(c):
        l, m = c // 2, c % 2
        src, dst = (w1, o1_hbm) if m == 0 else (w2, o2_hbm)
        return pltpu.make_async_copy(src.at[l], dst.at[l], io_sem.at[c])

    in_a = pltpu.make_async_copy(a_hbm, a_ref, io_sem.at[n_chunks])
    in_t = pltpu.make_async_copy(t_hbm, t_ref, io_sem.at[n_chunks + 1])
    for c in range(n_chunks):
        load_in(c).start()
    in_a.start()
    in_t.start()

    barrier = pltpu.get_barrier_semaphore()
    for k in range(log_g):
        pl.semaphore_signal(barrier, inc=1, device_id=as_id((me + n_dev - 2 ** k) % n_dev), device_id_type=MESH)

    def send(t, c):
        l, m = c // 2, c % 2
        peer = (me + two_power(t % log_g)) % n_dev
        src, dst = (q1, r1) if m == 0 else (q2, r2)
        return pltpu.make_async_remote_copy(
            src.at[t % 2, l], dst.at[t, l], send_sem.at[t % 2, c], recv_sem.at[t, c],
            device_id=as_id(peer), device_id_type=MESH)

    for c in range(n_chunks):
        l, m = c // 2, c % 2
        load_in(c).wait()
        if m == 0:
            q1[0, l] = w1[l].astype(jnp.bfloat16)
        else:
            q2[0, l] = w2[l].astype(jnp.bfloat16)
        if c == 0:
            pl.semaphore_wait(barrier, log_g)
        else:
            send(0, c - 1).start()
    in_a.wait()
    in_t.wait()

    row_dims = (((0,), (0,)), ((), ()))
    feat_dims = (((1,), (1,)), ((), ()))

    def step(t, carry):
        slot = t % 2
        nxt = 1 - slot
        self_w = mix_ref[t]
        peer_w = 1.0 - self_w
        hid = a_ref[t].astype(jnp.float32)
        for l in range(n_layers):
            inv = lax.rsqrt(jnp.mean(hid * hid, axis=-1, keepdims=True) + RMS_EPS)
            normed = (hid * inv).astype(jnp.bfloat16)
            z = jnp.dot(normed, q1[slot, l], preferred_element_type=jnp.float32)
            z2 = z * z
            th = jnp.tanh(z * (GELU_A + GELU_B * z2))
            half = 0.5 * z
            act = (half + half * th).astype(jnp.bfloat16)
            gs[l] = 0.5 + 0.5 * th + half * (1.0 - th * th) * (GELU_A + (3.0 * GELU_B) * z2)
            us[l] = act
            xs[l] = normed
            hs[l] = hid
            invs[l] = jnp.broadcast_to(inv, (rows, feat))
            out = jnp.dot(act, q2[slot, l], preferred_element_type=jnp.float32)
            hid = (hid + out).astype(jnp.bfloat16).astype(jnp.float32)
            if l == 0:
                send(t, n_chunks - 1).start()
        d_hid = (2.0 / (rows * feat)) * (hid - t_ref[t].astype(jnp.float32))
        for l in reversed(range(n_layers)):
            d_out = d_hid.astype(jnp.bfloat16)
            d_act = lax.dot_general(d_out, q2[slot, l], feat_dims, preferred_element_type=jnp.float32)
            d_pre = (d_act * gs[l]).astype(jnp.bfloat16)
            g2 = lax.dot_general(us[l], d_out, row_dims, preferred_element_type=jnp.float32)
            w2[l] = self_w * w2[l] - rate * g2
            if l > 0:
                d_norm = lax.dot_general(d_pre, q1[slot, l], feat_dims, preferred_element_type=jnp.float32)
                inv = invs[l]
                hid_l = hs[l]
                d_hid = d_hid + inv * d_norm - (inv * inv * inv) * hid_l * jnp.mean(d_norm * hid_l, axis=-1, keepdims=True)
            g1 = lax.dot_general(xs[l], d_pre, row_dims, preferred_element_type=jnp.float32)
            w1[l] = self_w * w1[l] - rate * g1

        more = t < n_steps - 1
        for c in range(n_chunks):
            l, m = c // 2, c % 2
            send(t, c).wait_recv()

            @pl.when(t > 0)
            def _():
                send(t - 1, c).wait_send()

            if m == 0:
                new = w1[l] + peer_w * r1[t, l].astype(jnp.float32)
                w1[l] = new
                q1[nxt, l] = new.astype(jnp.bfloat16)
            else:
                new = w2[l] + peer_w * r2[t, l].astype(jnp.float32)
                w2[l] = new
                q2[nxt, l] = new.astype(jnp.bfloat16)
            if c > 0:
                @pl.when(more)
                def _():
                    send(t + 1, c - 1).start()
        return carry

    lax.fori_loop(0, n_steps, step, 0)
    for c in range(n_chunks):
        load_out(c).start()
    for c in range(n_chunks):
        send(n_steps - 1, c).wait_send()
        load_out(c).wait()


def solution(mesh):
    n_inner = mesh.shape['inner']
    n_dev = mesh.shape['outer'] * n_inner
    spec = P('outer', 'inner')

    def device_run(w_one, w_two, inputs, targets, mix_self):
        n_layers, feat, wide = w_one.shape[2:]
        n_steps, rows = inputs.shape[2:4]
        bf, f32 = jnp.bfloat16, jnp.float32
        out_one, out_two = pl.pallas_call(
            lambda *refs: run_kernel(n_dev, n_inner, *refs),
            out_shape=(jax.ShapeDtypeStruct((n_layers, feat, wide), f32), jax.ShapeDtypeStruct((n_layers, wide, feat), f32)),
            in_specs=[pl.BlockSpec(memory_space=pltpu.SMEM)] + [pl.BlockSpec(memory_space=pl.ANY)] * 4,
            out_specs=(pl.BlockSpec(memory_space=pl.ANY),) * 2,
            scratch_shapes=[
                pltpu.VMEM((n_steps, rows, feat), bf), pltpu.VMEM((n_steps, rows, feat), bf),
                pltpu.VMEM((n_layers, feat, wide), f32), pltpu.VMEM((n_layers, wide, feat), f32),
                pltpu.VMEM((2, n_layers, feat, wide), bf), pltpu.VMEM((2, n_layers, wide, feat), bf),
                pltpu.VMEM((n_steps, n_layers, feat, wide), bf), pltpu.VMEM((n_steps, n_layers, wide, feat), bf),
                pltpu.VMEM((n_layers, rows, feat), bf), pltpu.VMEM((n_layers, rows, wide), bf),
                pltpu.VMEM((n_layers, rows, wide), f32), pltpu.VMEM((n_layers, rows, feat), f32),
                pltpu.VMEM((n_layers, rows, feat), f32),
                pltpu.SemaphoreType.DMA((2 * n_layers + 2,)), pltpu.SemaphoreType.DMA((2, 2 * n_layers)),
                pltpu.SemaphoreType.DMA((n_steps, 2 * n_layers)),
            ],
            compiler_params=pltpu.CompilerParams(collective_id=0, has_side_effects=True, vmem_limit_bytes=48 * 1024 * 1024),
            name="gossip_run",
        )(mix_self[0, 0], inputs[0, 0], targets[0, 0], w_one[0, 0], w_two[0, 0])
        return out_one[None, None], out_two[None, None]

    return jax.shard_map(device_run, mesh=mesh, in_specs=(spec,) * 5, out_specs=(spec, spec), check_vma=False)
```

```python
import jax
import jax.numpy as jnp
from jax import lax
from jax.experimental import pallas as pl
from jax.experimental.pallas import tpu as pltpu
from jax.sharding import PartitionSpec as P

RMS_EPS = 1e-6
RATE_BASE = 1.5
MESH = pl.DeviceIdType.MESH
GELU_A = 0.7978845608028654
GELU_B = 0.7978845608028654 * 0.044715

ROUTES = (
    {2: (2,) * 8, 4: (0, 1) * 4, 6: (0, 0, 0, 3) * 2, 7: (3,) * 8},
    {1: (1,) * 8, 2: (0, 1) * 4, 3: (0, 1, 0, 0) * 2, 4: (1, 0) * 4},
)
GATES = ((1, 1, 2), (1, 3, 4), (1, 5, 6), (1, 9, 10), (1, 11, 12), (1, 13, 14))
RELAY_AHEAD = 5


def two_power(k):
    return (1 + k % 2) * (1 + 3 * ((k // 2) % 2)) * (1 + 15 * (k // 4))


def run_kernel(n_dev, n_inner, mix_ref, a_hbm, t_hbm, w1_hbm, w2_hbm, o1_hbm, o2_hbm,
               a_ref, t_ref, w1, w2, q1, q2, r1, r2, p1, p2, xs, us, gs, hs, invs,
               io_sem, send_sem, recv_sem, pass_sem, pass_recv_sem, gate_sem):
    n_steps, rows, feat = a_ref.shape
    n_layers = w1.shape[0]
    log_g = n_dev.bit_length() - 1
    rate = RATE_BASE / n_layers
    me = lax.axis_index('outer') * n_inner + lax.axis_index('inner')
    core = me % 2
    plane_pos, line_pos = me % 32, me % 8
    n_chunks = 2 * n_layers

    def as_id(r):
        r = r % n_dev
        return (r // n_inner, r % n_inner)

    def load_in(c):
        l, m = c // 2, c % 2
        src, dst = (w1_hbm, w1) if m == 0 else (w2_hbm, w2)
        return pltpu.make_async_copy(src.at[l], dst.at[l], io_sem.at[c])

    def load_out(c):
        l, m = c // 2, c % 2
        src, dst = (w1, o1_hbm) if m == 0 else (w2, o2_hbm)
        return pltpu.make_async_copy(src.at[l], dst.at[l], io_sem.at[c])

    in_a = pltpu.make_async_copy(a_hbm, a_ref, io_sem.at[n_chunks])
    in_t = pltpu.make_async_copy(t_hbm, t_ref, io_sem.at[n_chunks + 1])
    for c in range(n_chunks):
        load_in(c).start()
    in_a.start()
    in_t.start()

    offsets = sorted({2 ** k for k in range(log_g)} | {2 ** k - 32 + n_dev for k in range(1, 5)}
                     | {2 ** k - 8 + n_dev for k in range(1, 3)} | {n_dev - 96, n_dev - 64})
    barrier = pltpu.get_barrier_semaphore()
    for off in offsets:
        pl.semaphore_signal(barrier, inc=1, device_id=as_id(me + n_dev - off), device_id_type=MESH)

    def kinds(k):
        out = [0] * n_chunks
        for cls in range(2):
            for step_k, row in ROUTES[cls].items():
                here = jnp.where((k == step_k) & (core == cls), 1, 0)
                out = [o + v * here if v else o for o, v in zip(out, row)]
        return out

    def own_buf(c):
        return (q1, r1, p1) if c % 2 == 0 else (q2, r2, p2)

    def start_send(t, k, shift, kind, c):
        l = c // 2
        own, final, relay = own_buf(c)

        def go(dst, sem, to):
            pltpu.make_async_remote_copy(own.at[t % 2, l], dst.at[t, l], send_sem.at[t % 2, c], sem.at[t, c],
                                         device_id=as_id(to), device_id_type=MESH).start()

        if isinstance(kind, int):
            go(final, recv_sem, me + shift)
            return
        via_plane = (kind == 1) & (plane_pos + shift >= 32)
        via_line = (kind == 2) & (line_pos + shift >= 8)
        via_back = kind == 3
        via = via_plane | via_line | via_back
        stop = jnp.where(via_plane, me + shift - 32, jnp.where(via_line, me + shift - 8, me - jnp.where(k == 6, 96, 64)))

        @pl.when(via)
        def _():
            go(relay, pass_recv_sem, stop + n_dev)

        @pl.when(jnp.logical_not(via))
        def _():
            go(final, recv_sem, me + shift)

    def wait_sent(t, c):
        own, final, _ = own_buf(c)
        pltpu.make_async_remote_copy(own.at[t % 2, c // 2], final.at[t, c // 2], send_sem.at[t % 2, c], recv_sem.at[t, c],
                                     device_id=as_id(me + 1), device_id_type=MESH).wait_send()

    def wait_arrived(t, c):
        own, final, _ = own_buf(c)
        pltpu.make_async_remote_copy(own.at[t % 2, c // 2], final.at[t, c // 2], send_sem.at[t % 2, c], recv_sem.at[t, c],
                                     device_id=as_id(me + 1), device_id_type=MESH).wait_recv()

    def pass_copy(t, c, to):
        _, final, relay = own_buf(c)
        return pltpu.make_async_remote_copy(relay.at[t, c // 2], final.at[t, c // 2], pass_sem.at[t % 2, c], recv_sem.at[t, c],
                                            device_id=as_id(to), device_id_type=MESH)

    def pass_in(t, c):
        _, final, relay = own_buf(c)
        return pltpu.make_async_remote_copy(relay.at[t, c // 2], relay.at[t, c // 2], pass_sem.at[t % 2, c], pass_recv_sem.at[t, c],
                                            device_id=as_id(me + 1), device_id_type=MESH)

    def pass_roles(k, shift, kind_row):
        out = []
        for kind in kind_row:
            if isinstance(kind, int):
                out.append(None)
                continue
            plane = (kind == 1) & (plane_pos < shift)
            line = (kind == 2) & (line_pos < shift)
            back = kind == 3
            to = me + jnp.where(plane, 32, jnp.where(line, 8, n_dev - jnp.where(k == 6, 96, 64)))
            out.append((jnp.where(plane | line | back, 1, 0), to))
        return out

    for c in range(n_chunks):
        l, m = c // 2, c % 2
        load_in(c).wait()
        if m == 0:
            q1[0, l] = w1[l].astype(jnp.bfloat16)
        else:
            q2[0, l] = w2[l].astype(jnp.bfloat16)
        if c == 0:
            pl.semaphore_wait(barrier, len(offsets))
        else:
            start_send(0, 0, 1, 0, c - 1)
    in_a.wait()
    in_t.wait()

    row_dims = (((0,), (0,)), ((), ()))
    feat_dims = (((1,), (1,)), ((), ()))

    def step(t, passed):
        slot = t % 2
        nxt = 1 - slot
        k = t % log_g
        k_next = (t + 1) % log_g
        shift, shift_next = two_power(k), two_power(k_next)
        kind_now, kind_next = kinds(k), kinds(k_next)
        self_w = mix_ref[t]
        peer_w = 1.0 - self_w
        hid = a_ref[t].astype(jnp.float32)
        for l in range(n_layers):
            inv = lax.rsqrt(jnp.mean(hid * hid, axis=-1, keepdims=True) + RMS_EPS)
            normed = (hid * inv).astype(jnp.bfloat16)
            z = jnp.dot(normed, q1[slot, l], preferred_element_type=jnp.float32)
            z2 = z * z
            th = jnp.tanh(z * (GELU_A + GELU_B * z2))
            half = 0.5 * z
            act = (half + half * th).astype(jnp.bfloat16)
            gs[l] = 0.5 + 0.5 * th + half * (1.0 - th * th) * (GELU_A + (3.0 * GELU_B) * z2)
            us[l] = act
            xs[l] = normed
            hs[l] = hid
            invs[l] = jnp.broadcast_to(inv, (rows, feat))
            out = jnp.dot(act, q2[slot, l], preferred_element_type=jnp.float32)
            hid = (hid + out).astype(jnp.bfloat16).astype(jnp.float32)
            if l == 0:
                start_send(t, k, shift, kind_now[n_chunks - 1], n_chunks - 1)
        d_hid = (2.0 / (rows * feat)) * (hid - t_ref[t].astype(jnp.float32))
        for l in reversed(range(n_layers)):
            d_out = d_hid.astype(jnp.bfloat16)
            d_act = lax.dot_general(d_out, q2[slot, l], feat_dims, preferred_element_type=jnp.float32)
            d_pre = (d_act * gs[l]).astype(jnp.bfloat16)
            g2 = lax.dot_general(us[l], d_out, row_dims, preferred_element_type=jnp.float32)
            w2[l] = self_w * w2[l] - rate * g2
            if l > 0:
                d_norm = lax.dot_general(d_pre, q1[slot, l], feat_dims, preferred_element_type=jnp.float32)
                inv = invs[l]
                hid_l = hs[l]
                d_hid = d_hid + inv * d_norm - (inv * inv * inv) * hid_l * jnp.mean(d_norm * hid_l, axis=-1, keepdims=True)
            g1 = lax.dot_general(xs[l], d_pre, row_dims, preferred_element_type=jnp.float32)
            w1[l] = self_w * w1[l] - rate * g1

        more = t < n_steps - 1
        roles = pass_roles(k, shift, kind_now)

        def pass_on(c):
            if roles[c] is None:
                return
            role, to = roles[c]

            @pl.when(role == 1)
            def _():
                pass_in(t, c).wait_recv()
                pass_copy(t, c, to).start()

        for c in range(min(RELAY_AHEAD, n_chunks)):
            pass_on(c)
        for c in range(n_chunks):
            l, m = c // 2, c % 2
            if c + RELAY_AHEAD < n_chunks:
                pass_on(c + RELAY_AHEAD)
            wait_arrived(t, c)

            @pl.when(t > 0)
            def _():
                wait_sent(t - 1, c)

            if m == 0:
                new = w1[l] + peer_w * r1[t, l].astype(jnp.float32)
                w1[l] = new
                q1[nxt, l] = new.astype(jnp.bfloat16)
            else:
                new = w2[l] + peer_w * r2[t, l].astype(jnp.float32)
                w2[l] = new
                q2[nxt, l] = new.astype(jnp.bfloat16)
            if c == 1:
                for i, (cls, at, other) in enumerate(GATES):
                    @pl.when((core == cls) & (t + 1 == at))
                    def _():
                        pl.semaphore_wait(gate_sem.at[i], 1)
            if c > 0:
                @pl.when(more)
                def _():
                    start_send(t + 1, k_next, shift_next, kind_next[c - 1], c - 1)
        for i, (cls, at, other) in enumerate(GATES):
            @pl.when((core == 1 - cls) & (t == other))
            def _():
                pl.semaphore_signal(gate_sem.at[i], inc=1, device_id=as_id(me + 1 - 2 * core + n_dev), device_id_type=MESH)
        left = []
        for c in range(n_chunks):
            if roles[c] is None:
                continue

            @pl.when(passed[len(left)] == 1)
            def _():
                pass_copy(t - 1, c, me + 1).wait_send()

            left.append(roles[c][0])
        return tuple(left)

    n_pass = sum(1 for c in range(n_chunks) if any(row[c] for rows_ in ROUTES for row in rows_.values()))
    passed = lax.fori_loop(0, n_steps, step, (jnp.int32(0),) * n_pass)
    i = 0
    for c in range(n_chunks):
        load_out(c).start()
    for c in range(n_chunks):
        if any(row[c] for rows_ in ROUTES for row in rows_.values()):
            @pl.when(passed[i] == 1)
            def _():
                pass_copy(n_steps - 1, c, me + 1).wait_send()
            i += 1
        wait_sent(n_steps - 1, c)
        load_out(c).wait()


def solution(mesh):
    n_inner = mesh.shape['inner']
    n_dev = mesh.shape['outer'] * n_inner
    spec = P('outer', 'inner')

    def device_run(w_one, w_two, inputs, targets, mix_self):
        n_layers, feat, wide = w_one.shape[2:]
        n_steps, rows = inputs.shape[2:4]
        bf, f32 = jnp.bfloat16, jnp.float32
        out_one, out_two = pl.pallas_call(
            lambda *refs: run_kernel(n_dev, n_inner, *refs),
            out_shape=(jax.ShapeDtypeStruct((n_layers, feat, wide), f32), jax.ShapeDtypeStruct((n_layers, wide, feat), f32)),
            in_specs=[pl.BlockSpec(memory_space=pltpu.SMEM)] + [pl.BlockSpec(memory_space=pl.ANY)] * 4,
            out_specs=(pl.BlockSpec(memory_space=pl.ANY),) * 2,
            scratch_shapes=[
                pltpu.VMEM((n_steps, rows, feat), bf), pltpu.VMEM((n_steps, rows, feat), bf),
                pltpu.VMEM((n_layers, feat, wide), f32), pltpu.VMEM((n_layers, wide, feat), f32),
                pltpu.VMEM((2, n_layers, feat, wide), bf), pltpu.VMEM((2, n_layers, wide, feat), bf),
                pltpu.VMEM((n_steps, n_layers, feat, wide), bf), pltpu.VMEM((n_steps, n_layers, wide, feat), bf),
                pltpu.VMEM((n_steps, n_layers, feat, wide), bf), pltpu.VMEM((n_steps, n_layers, wide, feat), bf),
                pltpu.VMEM((n_layers, rows, feat), bf), pltpu.VMEM((n_layers, rows, wide), bf),
                pltpu.VMEM((n_layers, rows, wide), f32), pltpu.VMEM((n_layers, rows, feat), f32),
                pltpu.VMEM((n_layers, rows, feat), f32),
                pltpu.SemaphoreType.DMA((2 * n_layers + 2,)), pltpu.SemaphoreType.DMA((2, 2 * n_layers)),
                pltpu.SemaphoreType.DMA((n_steps, 2 * n_layers)), pltpu.SemaphoreType.DMA((2, 2 * n_layers)),
                pltpu.SemaphoreType.DMA((n_steps, 2 * n_layers)), pltpu.SemaphoreType.REGULAR((len(GATES),)),
            ],
            compiler_params=pltpu.CompilerParams(collective_id=0, has_side_effects=True, vmem_limit_bytes=63 * 1024 * 1024),
            name="gossip_run",
        )(mix_self[0, 0], inputs[0, 0], targets[0, 0], w_one[0, 0], w_two[0, 0])
        return out_one[None, None], out_two[None, None]

    return jax.shard_map(device_run, mesh=mesh, in_specs=(spec,) * 5, out_specs=(spec, spec), check_vma=False)
```

```python
import jax
import jax.numpy as jnp
from jax import lax
from jax.experimental import pallas as pl
from jax.experimental.pallas import tpu as pltpu
from jax.sharding import PartitionSpec as P

RMS_EPS = 1e-6
RATE_BASE = 1.5
MESH = pl.DeviceIdType.MESH
GELU_A = 0.7978845608028654
GELU_B = 0.7978845608028654 * 0.044715

ROUTES = (
    {1: (0, 0, 0, 0, 1, 0, 0, 0), 2: (0, 4, 0, 0, 4, 0, 4, 0), 3: (1, 0, 1, 0, 1, 1, 0, 1), 6: (0, 0, 0, 3, 0, 0, 0, 3), 7: (3, 3, 3, 0, 3, 3, 3, 3)},
    {1: (4, 4, 1, 0, 4, 4, 4, 4), 2: (2, 4, 2, 4, 2, 4, 2, 4), 3: (1, 0, 1, 0, 1, 1, 0, 1), 4: (0, 1, 0, 0, 0, 1, 0, 1)},
)
GATES = ((1, 1, 2), (1, 3, 4), (1, 4, 6), (1, 5, 5), (1, 7, 7), (1, 9, 10), (1, 11, 11), (1, 12, 13), (1, 13, 12))
RELAY_AHEAD = 5


def two_power(k):
    return (1 + k % 2) * (1 + 3 * ((k // 2) % 2)) * (1 + 15 * (k // 4))


def run_kernel(n_dev, n_inner, mix_ref, a_hbm, t_hbm, w1_hbm, w2_hbm, o1_hbm, o2_hbm,
               a_ref, t_ref, w1, w2, q1, q2, r1, r2, p1, p2, xs, us, gs, hs, invs,
               io_sem, send_sem, recv_sem, pass_sem, pass_recv_sem, gate_sem):
    n_steps, rows, feat = a_ref.shape
    n_layers = w1.shape[0]
    log_g = n_dev.bit_length() - 1
    rate = RATE_BASE / n_layers
    me = lax.axis_index('outer') * n_inner + lax.axis_index('inner')
    core = me % 2
    plane_pos, line_pos = me % 32, me % 8
    n_chunks = 2 * n_layers

    def as_id(r):
        r = r % n_dev
        return (r // n_inner, r % n_inner)

    def load_in(c):
        l, m = c // 2, c % 2
        src, dst = (w1_hbm, w1) if m == 0 else (w2_hbm, w2)
        return pltpu.make_async_copy(src.at[l], dst.at[l], io_sem.at[c])

    def load_out(c):
        l, m = c // 2, c % 2
        src, dst = (w1, o1_hbm) if m == 0 else (w2, o2_hbm)
        return pltpu.make_async_copy(src.at[l], dst.at[l], io_sem.at[c])

    in_a = pltpu.make_async_copy(a_hbm, a_ref, io_sem.at[n_chunks])
    in_t = pltpu.make_async_copy(t_hbm, t_ref, io_sem.at[n_chunks + 1])
    for c in range(n_chunks):
        load_in(c).start()
    in_a.start()
    in_t.start()

    offsets = sorted({2 ** k for k in range(log_g)} | {2 ** k - 32 + n_dev for k in range(1, 5)}
                     | {2 ** k - 8 + n_dev for k in range(1, 3)} | {n_dev - 96, n_dev - 64} | {n_dev - 24}
                     | {2 ** k - 8 + 32 for k in range(1, 3)})
    barrier = pltpu.get_barrier_semaphore()
    for off in offsets:
        pl.semaphore_signal(barrier, inc=1, device_id=as_id(me + n_dev - off), device_id_type=MESH)

    def kinds(k):
        out = [0] * n_chunks
        for cls in range(2):
            for step_k, row in ROUTES[cls].items():
                here = jnp.where((k == step_k) & (core == cls), 1, 0)
                out = [o + v * here if v else o for o, v in zip(out, row)]
        return out

    def own_buf(c):
        return (q1, r1, p1) if c % 2 == 0 else (q2, r2, p2)

    def start_send(t, k, shift, kind, c):
        l = c // 2
        own, final, relay = own_buf(c)

        def go(dst, sem, to):
            pltpu.make_async_remote_copy(own.at[t % 2, l], dst.at[t, l], send_sem.at[t % 2, c], sem.at[t, c],
                                         device_id=as_id(to), device_id_type=MESH).start()

        if isinstance(kind, int):
            go(final, recv_sem, me + shift)
            return
        via_plane = (kind == 1) & (plane_pos + shift >= 32)
        via_line = (kind == 2) & (line_pos + shift >= 8)
        via_back = kind == 3
        via_row = (kind == 4) & (line_pos + shift >= 8)
        via = via_plane | via_line | via_back | via_row
        stop = jnp.where(via_plane, me + shift - 32, jnp.where(via_line, me + shift - 8, me - jnp.where(k == 6, 96, 64)))
        stop = jnp.where(via_row, me - plane_pos + (plane_pos + 8) % 32, stop)

        @pl.when(via)
        def _():
            go(relay, pass_recv_sem, stop + n_dev)

        @pl.when(jnp.logical_not(via))
        def _():
            go(final, recv_sem, me + shift)

    def wait_sent(t, c):
        own, final, _ = own_buf(c)
        pltpu.make_async_remote_copy(own.at[t % 2, c // 2], final.at[t, c // 2], send_sem.at[t % 2, c], recv_sem.at[t, c],
                                     device_id=as_id(me + 1), device_id_type=MESH).wait_send()

    def wait_arrived(t, c):
        own, final, _ = own_buf(c)
        pltpu.make_async_remote_copy(own.at[t % 2, c // 2], final.at[t, c // 2], send_sem.at[t % 2, c], recv_sem.at[t, c],
                                     device_id=as_id(me + 1), device_id_type=MESH).wait_recv()

    def pass_copy(t, c, to):
        _, final, relay = own_buf(c)
        return pltpu.make_async_remote_copy(relay.at[t, c // 2], final.at[t, c // 2], pass_sem.at[t % 2, c], recv_sem.at[t, c],
                                            device_id=as_id(to), device_id_type=MESH)

    def pass_in(t, c):
        _, final, relay = own_buf(c)
        return pltpu.make_async_remote_copy(relay.at[t, c // 2], relay.at[t, c // 2], pass_sem.at[t % 2, c], pass_recv_sem.at[t, c],
                                            device_id=as_id(me + 1), device_id_type=MESH)

    def pass_roles(k, shift, kind_row):
        out = []
        for kind in kind_row:
            if isinstance(kind, int):
                out.append(None)
                continue
            plane = (kind == 1) & (plane_pos < shift)
            line = (kind == 2) & (line_pos < shift)
            back = kind == 3
            row = (kind == 4) & (line_pos + shift >= 8)
            to = me + jnp.where(plane, 32, jnp.where(line, 8, n_dev - jnp.where(k == 6, 96, 64)))
            to = jnp.where(row, me + shift - 8 + jnp.where(plane_pos < 8, 32, 0), to)
            out.append((jnp.where(plane | line | back | row, 1, 0), to))
        return out

    for c in range(n_chunks):
        l, m = c // 2, c % 2
        load_in(c).wait()
        if m == 0:
            q1[0, l] = w1[l].astype(jnp.bfloat16)
        else:
            q2[0, l] = w2[l].astype(jnp.bfloat16)
        if c == 0:
            pl.semaphore_wait(barrier, len(offsets))
        else:
            start_send(0, 0, 1, 0, c - 1)
    in_a.wait()
    in_t.wait()

    row_dims = (((0,), (0,)), ((), ()))
    feat_dims = (((1,), (1,)), ((), ()))

    def step(t, passed):
        slot = t % 2
        nxt = 1 - slot
        k = t % log_g
        k_next = (t + 1) % log_g
        shift, shift_next = two_power(k), two_power(k_next)
        kind_now, kind_next = kinds(k), kinds(k_next)
        self_w = mix_ref[t]
        peer_w = 1.0 - self_w
        hid = a_ref[t].astype(jnp.float32)
        for l in range(n_layers):
            inv = lax.rsqrt(jnp.mean(hid * hid, axis=-1, keepdims=True) + RMS_EPS)
            normed = (hid * inv).astype(jnp.bfloat16)
            z = jnp.dot(normed, q1[slot, l], preferred_element_type=jnp.float32)
            z2 = z * z
            th = jnp.tanh(z * (GELU_A + GELU_B * z2))
            half = 0.5 * z
            act = (half + half * th).astype(jnp.bfloat16)
            gs[l] = 0.5 + 0.5 * th + half * (1.0 - th * th) * (GELU_A + (3.0 * GELU_B) * z2)
            us[l] = act
            xs[l] = normed
            hs[l] = hid
            invs[l] = jnp.broadcast_to(inv, (rows, feat))
            out = jnp.dot(act, q2[slot, l], preferred_element_type=jnp.float32)
            hid = (hid + out).astype(jnp.bfloat16).astype(jnp.float32)
            if l == 0:
                start_send(t, k, shift, kind_now[n_chunks - 1], n_chunks - 1)
        d_hid = (2.0 / (rows * feat)) * (hid - t_ref[t].astype(jnp.float32))
        for l in reversed(range(n_layers)):
            d_out = d_hid.astype(jnp.bfloat16)
            d_act = lax.dot_general(d_out, q2[slot, l], feat_dims, preferred_element_type=jnp.float32)
            d_pre = (d_act * gs[l]).astype(jnp.bfloat16)
            g2 = lax.dot_general(us[l], d_out, row_dims, preferred_element_type=jnp.float32)
            w2[l] = self_w * w2[l] - rate * g2
            if l > 0:
                d_norm = lax.dot_general(d_pre, q1[slot, l], feat_dims, preferred_element_type=jnp.float32)
                inv = invs[l]
                hid_l = hs[l]
                d_hid = d_hid + inv * d_norm - (inv * inv * inv) * hid_l * jnp.mean(d_norm * hid_l, axis=-1, keepdims=True)
            g1 = lax.dot_general(xs[l], d_pre, row_dims, preferred_element_type=jnp.float32)
            w1[l] = self_w * w1[l] - rate * g1

        more = t < n_steps - 1
        roles = pass_roles(k, shift, kind_now)

        def pass_on(c):
            if roles[c] is None:
                return
            role, to = roles[c]

            @pl.when(role == 1)
            def _():
                pass_in(t, c).wait_recv()
                pass_copy(t, c, to).start()

        for c in range(min(RELAY_AHEAD, n_chunks)):
            pass_on(c)
        for c in range(n_chunks):
            l, m = c // 2, c % 2
            if c + RELAY_AHEAD < n_chunks:
                pass_on(c + RELAY_AHEAD)
            wait_arrived(t, c)

            @pl.when(t > 0)
            def _():
                wait_sent(t - 1, c)

            if m == 0:
                new = w1[l] + peer_w * r1[t, l].astype(jnp.float32)
                w1[l] = new
                q1[nxt, l] = new.astype(jnp.bfloat16)
            else:
                new = w2[l] + peer_w * r2[t, l].astype(jnp.float32)
                w2[l] = new
                q2[nxt, l] = new.astype(jnp.bfloat16)
            if c == 1:
                for i, (cls, at, other) in enumerate(GATES):
                    @pl.when((core == cls) & (t + 1 == at))
                    def _():
                        pl.semaphore_wait(gate_sem.at[i], 1)
            if c > 0:
                @pl.when(more)
                def _():
                    start_send(t + 1, k_next, shift_next, kind_next[c - 1], c - 1)
        for i, (cls, at, other) in enumerate(GATES):
            @pl.when((core == 1 - cls) & (t == other))
            def _():
                pl.semaphore_signal(gate_sem.at[i], inc=1, device_id=as_id(me + 1 - 2 * core + n_dev), device_id_type=MESH)
        left = []
        for c in range(n_chunks):
            if roles[c] is None:
                continue

            @pl.when(passed[len(left)] == 1)
            def _():
                pass_copy(t - 1, c, me + 1).wait_send()

            left.append(roles[c][0])
        return tuple(left)

    n_pass = sum(1 for c in range(n_chunks) if any(row[c] for rows_ in ROUTES for row in rows_.values()))
    passed = lax.fori_loop(0, n_steps, step, (jnp.int32(0),) * n_pass)
    i = 0
    for c in range(n_chunks):
        load_out(c).start()
    for c in range(n_chunks):
        if any(row[c] for rows_ in ROUTES for row in rows_.values()):
            @pl.when(passed[i] == 1)
            def _():
                pass_copy(n_steps - 1, c, me + 1).wait_send()
            i += 1
        wait_sent(n_steps - 1, c)
        load_out(c).wait()


def solution(mesh):
    n_inner = mesh.shape['inner']
    n_dev = mesh.shape['outer'] * n_inner
    spec = P('outer', 'inner')

    def device_run(w_one, w_two, inputs, targets, mix_self):
        n_layers, feat, wide = w_one.shape[2:]
        n_steps, rows = inputs.shape[2:4]
        bf, f32 = jnp.bfloat16, jnp.float32
        out_one, out_two = pl.pallas_call(
            lambda *refs: run_kernel(n_dev, n_inner, *refs),
            out_shape=(jax.ShapeDtypeStruct((n_layers, feat, wide), f32), jax.ShapeDtypeStruct((n_layers, wide, feat), f32)),
            in_specs=[pl.BlockSpec(memory_space=pltpu.SMEM)] + [pl.BlockSpec(memory_space=pl.ANY)] * 4,
            out_specs=(pl.BlockSpec(memory_space=pl.ANY),) * 2,
            scratch_shapes=[
                pltpu.VMEM((n_steps, rows, feat), bf), pltpu.VMEM((n_steps, rows, feat), bf),
                pltpu.VMEM((n_layers, feat, wide), f32), pltpu.VMEM((n_layers, wide, feat), f32),
                pltpu.VMEM((2, n_layers, feat, wide), bf), pltpu.VMEM((2, n_layers, wide, feat), bf),
                pltpu.VMEM((n_steps, n_layers, feat, wide), bf), pltpu.VMEM((n_steps, n_layers, wide, feat), bf),
                pltpu.VMEM((n_steps, n_layers, feat, wide), bf), pltpu.VMEM((n_steps, n_layers, wide, feat), bf),
                pltpu.VMEM((n_layers, rows, feat), bf), pltpu.VMEM((n_layers, rows, wide), bf),
                pltpu.VMEM((n_layers, rows, wide), f32), pltpu.VMEM((n_layers, rows, feat), f32),
                pltpu.VMEM((n_layers, rows, feat), f32),
                pltpu.SemaphoreType.DMA((2 * n_layers + 2,)), pltpu.SemaphoreType.DMA((2, 2 * n_layers)),
                pltpu.SemaphoreType.DMA((n_steps, 2 * n_layers)), pltpu.SemaphoreType.DMA((2, 2 * n_layers)),
                pltpu.SemaphoreType.DMA((n_steps, 2 * n_layers)), pltpu.SemaphoreType.REGULAR((len(GATES),)),
            ],
            compiler_params=pltpu.CompilerParams(collective_id=0, has_side_effects=True, vmem_limit_bytes=63 * 1024 * 1024),
            name="gossip_run",
        )(mix_self[0, 0], inputs[0, 0], targets[0, 0], w_one[0, 0], w_two[0, 0])
        return out_one[None, None], out_two[None, None]

    return jax.shard_map(device_run, mesh=mesh, in_specs=(spec,) * 5, out_specs=(spec, spec), check_vma=False)
```

```python
import jax
import jax.numpy as jnp
from jax import lax
from jax.experimental import pallas as pl
from jax.experimental.pallas import tpu as pltpu
from jax.sharding import PartitionSpec as P

RMS_EPS = 1e-6
RATE_BASE = 1.5
MESH = pl.DeviceIdType.MESH
GELU_A = 0.7978845608028654
GELU_B = 0.7978845608028654 * 0.044715

ROUTES = (
    {1: (0, 4, 0, 0, 0, 0, 0, 0), 2: (4, 4, 4, 4, 4, 4, 4, 4), 3: (0, 0, 0, 0, 1, 0, 0, 0), 4: (1, 1, 1, 1, 1, 1, 1, 1), 9: (0, 4, 0, 0, 0, 0, 0, 0), 10: (4, 4, 4, 4, 4, 4, 4, 4), 11: (1, 1, 0, 0, 1, 0, 1, 0)},
    {1: (0, 4, 0, 0, 0, 0, 0, 0), 2: (1, 1, 1, 1, 1, 1, 1, 1), 3: (0, 0, 0, 1, 1, 0, 0, 0), 4: (1, 1, 1, 1, 1, 1, 1, 1), 6: (0, 3, 0, 0, 0, 3, 0, 0), 7: (3, 3, 3, 3, 3, 3, 3, 3), 9: (0, 4, 0, 0, 0, 0, 0, 0), 10: (1, 1, 1, 1, 1, 1, 1, 1), 11: (0, 0, 0, 0, 1, 0, 0, 0), 14: (0, 3, 0, 0, 0, 3, 0, 0), 15: (3, 3, 3, 3, 3, 3, 0, 3)},
)
GATES = ((0, 1, 2), (0, 2, 3), (0, 3, 4), (0, 7, 6), (0, 9, 10), (0, 10, 11), (0, 13, 12), (0, 15, 14))
RELAY_AHEAD = 7


def two_power(k):
    return (1 + k % 2) * (1 + 3 * ((k // 2) % 2)) * (1 + 15 * (k // 4))


def run_kernel(n_dev, n_inner, mix_ref, a_hbm, t_hbm, w1_hbm, w2_hbm, o1_hbm, o2_hbm,
               a_ref, t_ref, w1, w2, q1, q2, r1, r2, p1, p2, xs, us, gs, hs, invs,
               io_sem, send_sem, recv_sem, pass_sem, pass_recv_sem, gate_sem):
    n_steps, rows, feat = a_ref.shape
    n_layers = w1.shape[0]
    log_g = n_dev.bit_length() - 1
    rate = RATE_BASE / n_layers
    me = lax.axis_index('outer') * n_inner + lax.axis_index('inner')
    core = me % 2
    plane_pos, line_pos = me % 32, me % 8
    n_chunks = 2 * n_layers

    def as_id(r):
        r = r % n_dev
        return (r // n_inner, r % n_inner)

    def load_in(c):
        l, m = c // 2, c % 2
        src, dst = (w1_hbm, w1) if m == 0 else (w2_hbm, w2)
        return pltpu.make_async_copy(src.at[l], dst.at[l], io_sem.at[c])

    def load_out(c):
        l, m = c // 2, c % 2
        src, dst = (w1, o1_hbm) if m == 0 else (w2, o2_hbm)
        return pltpu.make_async_copy(src.at[l], dst.at[l], io_sem.at[c])

    in_a = pltpu.make_async_copy(a_hbm, a_ref, io_sem.at[n_chunks])
    in_t = pltpu.make_async_copy(t_hbm, t_ref, io_sem.at[n_chunks + 1])
    for c in range(n_chunks):
        load_in(c).start()
    in_a.start()
    in_t.start()

    offsets = sorted({2 ** k for k in range(log_g)} | {2 ** k - 32 + n_dev for k in range(1, 5)}
                     | {2 ** k - 8 + n_dev for k in range(1, 3)} | {n_dev - 96, n_dev - 64} | {n_dev - 24}
                     | {2 ** k - 8 + 32 for k in range(1, 3)})
    barrier = pltpu.get_barrier_semaphore()
    for off in offsets:
        pl.semaphore_signal(barrier, inc=1, device_id=as_id(me + n_dev - off), device_id_type=MESH)

    def kinds(t):
        out = [0] * n_chunks
        for cls in range(2):
            for at, row in ROUTES[cls].items():
                here = jnp.where((t == at) & (core == cls), 1, 0)
                out = [o + v * here if v else o for o, v in zip(out, row)]
        return out

    def own_buf(c):
        return (q1, r1, p1) if c % 2 == 0 else (q2, r2, p2)

    def start_send(t, k, shift, kind, c):
        l = c // 2
        own, final, relay = own_buf(c)

        def go(dst, sem, to):
            pltpu.make_async_remote_copy(own.at[t % 2, l], dst.at[t, l], send_sem.at[t % 2, c], sem.at[t, c],
                                         device_id=as_id(to), device_id_type=MESH).start()

        if isinstance(kind, int):
            go(final, recv_sem, me + shift)
            return
        via_plane = (kind == 1) & (plane_pos + shift >= 32)
        via_line = (kind == 2) & (line_pos + shift >= 8)
        via_back = kind == 3
        via_row = (kind == 4) & (line_pos + shift >= 8)
        via_two = kind == 5
        via = via_plane | via_line | via_back | via_row | via_two
        stop = jnp.where(via_plane, me + shift - 32, jnp.where(via_line, me + shift - 8, me - jnp.where(k == 6, 96, 64)))
        stop = jnp.where(via_two, me + 64, stop)
        stop = jnp.where(via_row, me - plane_pos + (plane_pos + 8) % 32, stop)

        @pl.when(via)
        def _():
            go(relay, pass_recv_sem, stop + n_dev)

        @pl.when(jnp.logical_not(via))
        def _():
            go(final, recv_sem, me + shift)

    def wait_sent(t, c):
        own, final, _ = own_buf(c)
        pltpu.make_async_remote_copy(own.at[t % 2, c // 2], final.at[t, c // 2], send_sem.at[t % 2, c], recv_sem.at[t, c],
                                     device_id=as_id(me + 1), device_id_type=MESH).wait_send()

    def wait_arrived(t, c):
        own, final, _ = own_buf(c)
        pltpu.make_async_remote_copy(own.at[t % 2, c // 2], final.at[t, c // 2], send_sem.at[t % 2, c], recv_sem.at[t, c],
                                     device_id=as_id(me + 1), device_id_type=MESH).wait_recv()

    def pass_copy(t, c, to):
        _, final, relay = own_buf(c)
        return pltpu.make_async_remote_copy(relay.at[t, c // 2], final.at[t, c // 2], pass_sem.at[t % 2, c], recv_sem.at[t, c],
                                            device_id=as_id(to), device_id_type=MESH)

    def pass_in(t, c):
        _, final, relay = own_buf(c)
        return pltpu.make_async_remote_copy(relay.at[t, c // 2], relay.at[t, c // 2], pass_sem.at[t % 2, c], pass_recv_sem.at[t, c],
                                            device_id=as_id(me + 1), device_id_type=MESH)

    def pass_roles(k, shift, kind_row):
        out = []
        for kind in kind_row:
            if isinstance(kind, int):
                out.append(None)
                continue
            plane = (kind == 1) & (plane_pos < shift)
            line = (kind == 2) & (line_pos < shift)
            back = kind == 3
            row = (kind == 4) & (line_pos + shift >= 8)
            to = me + jnp.where(plane, 32, jnp.where(line, 8, n_dev - jnp.where(k == 6, 96, 64)))
            two = kind == 5
            to = jnp.where(two, me + 64, to)
            to = jnp.where(row, me + shift - 8 + jnp.where(plane_pos < 8, 32, 0), to)
            out.append((jnp.where(plane | line | back | row | two, 1, 0), to))
        return out

    for c in range(n_chunks):
        l, m = c // 2, c % 2
        load_in(c).wait()
        if m == 0:
            q1[0, l] = w1[l].astype(jnp.bfloat16)
        else:
            q2[0, l] = w2[l].astype(jnp.bfloat16)
        if c == 0:
            pl.semaphore_wait(barrier, len(offsets))
        else:
            start_send(0, 0, 1, 0, c - 1)
    in_a.wait()
    in_t.wait()

    row_dims = (((0,), (0,)), ((), ()))
    feat_dims = (((1,), (1,)), ((), ()))

    def step(t, passed):
        slot = t % 2
        nxt = 1 - slot
        k = t % log_g
        k_next = (t + 1) % log_g
        shift, shift_next = two_power(k), two_power(k_next)
        kind_now, kind_next = kinds(t), kinds(t + 1)
        self_w = mix_ref[t]
        peer_w = 1.0 - self_w
        hid = a_ref[t].astype(jnp.float32)
        for l in range(n_layers):
            inv = lax.rsqrt(jnp.mean(hid * hid, axis=-1, keepdims=True) + RMS_EPS)
            normed = (hid * inv).astype(jnp.bfloat16)
            z = jnp.dot(normed, q1[slot, l], preferred_element_type=jnp.float32)
            z2 = z * z
            th = jnp.tanh(z * (GELU_A + GELU_B * z2))
            half = 0.5 * z
            act = (half + half * th).astype(jnp.bfloat16)
            gs[l] = 0.5 + 0.5 * th + half * (1.0 - th * th) * (GELU_A + (3.0 * GELU_B) * z2)
            us[l] = act
            xs[l] = normed
            hs[l] = hid
            invs[l] = jnp.broadcast_to(inv, (rows, feat))
            out = jnp.dot(act, q2[slot, l], preferred_element_type=jnp.float32)
            hid = (hid + out).astype(jnp.bfloat16).astype(jnp.float32)
            if l == 0:
                start_send(t, k, shift, kind_now[n_chunks - 1], n_chunks - 1)
        d_hid = (2.0 / (rows * feat)) * (hid - t_ref[t].astype(jnp.float32))
        for l in reversed(range(n_layers)):
            d_out = d_hid.astype(jnp.bfloat16)
            d_act = lax.dot_general(d_out, q2[slot, l], feat_dims, preferred_element_type=jnp.float32)
            d_pre = (d_act * gs[l]).astype(jnp.bfloat16)
            g2 = lax.dot_general(us[l], d_out, row_dims, preferred_element_type=jnp.float32)
            w2[l] = self_w * w2[l] - rate * g2
            if l > 0:
                d_norm = lax.dot_general(d_pre, q1[slot, l], feat_dims, preferred_element_type=jnp.float32)
                inv = invs[l]
                hid_l = hs[l]
                d_hid = d_hid + inv * d_norm - (inv * inv * inv) * hid_l * jnp.mean(d_norm * hid_l, axis=-1, keepdims=True)
            g1 = lax.dot_general(xs[l], d_pre, row_dims, preferred_element_type=jnp.float32)
            w1[l] = self_w * w1[l] - rate * g1

        more = t < n_steps - 1
        roles = pass_roles(k, shift, kind_now)

        def pass_on(c):
            if roles[c] is None:
                return
            role, to = roles[c]

            @pl.when(role == 1)
            def _():
                pass_in(t, c).wait_recv()
                pass_copy(t, c, to).start()

        for c in range(min(RELAY_AHEAD, n_chunks)):
            pass_on(c)
        for c in range(n_chunks):
            l, m = c // 2, c % 2
            if c + RELAY_AHEAD < n_chunks:
                pass_on(c + RELAY_AHEAD)
            wait_arrived(t, c)

            @pl.when(t > 0)
            def _():
                wait_sent(t - 1, c)

            if m == 0:
                new = w1[l] + peer_w * r1[t, l].astype(jnp.float32)
                w1[l] = new
                q1[nxt, l] = new.astype(jnp.bfloat16)
            else:
                new = w2[l] + peer_w * r2[t, l].astype(jnp.float32)
                w2[l] = new
                q2[nxt, l] = new.astype(jnp.bfloat16)
            if c == 1:
                for i, (cls, at, other) in enumerate(GATES):
                    @pl.when((core == cls) & (t + 1 == at))
                    def _():
                        pl.semaphore_wait(gate_sem.at[i], 1)
            if c > 0:
                @pl.when(more)
                def _():
                    start_send(t + 1, k_next, shift_next, kind_next[c - 1], c - 1)

                @pl.when(jnp.logical_not(more))
                def _():
                    load_out(c - 1).start()
        for i, (cls, at, other) in enumerate(GATES):
            @pl.when((core == 1 - cls) & (t == other))
            def _():
                pl.semaphore_signal(gate_sem.at[i], inc=1, device_id=as_id(me + 1 - 2 * core + n_dev), device_id_type=MESH)
        left = []
        for c in range(n_chunks):
            if roles[c] is None:
                continue

            @pl.when(passed[len(left)] == 1)
            def _():
                pass_copy(t - 1, c, me + 1).wait_send()

            left.append(roles[c][0])
        return tuple(left)

    n_pass = sum(1 for c in range(n_chunks) if any(row[c] for rows_ in ROUTES for row in rows_.values()))
    passed = lax.fori_loop(0, n_steps, step, (jnp.int32(0),) * n_pass)
    i = 0
    load_out(n_chunks - 1).start()
    for c in range(n_chunks):
        if any(row[c] for rows_ in ROUTES for row in rows_.values()):
            @pl.when(passed[i] == 1)
            def _():
                pass_copy(n_steps - 1, c, me + 1).wait_send()
            i += 1
        wait_sent(n_steps - 1, c)
        load_out(c).wait()


def solution(mesh):
    n_inner = mesh.shape['inner']
    n_dev = mesh.shape['outer'] * n_inner
    spec = P('outer', 'inner')

    def device_run(w_one, w_two, inputs, targets, mix_self):
        n_layers, feat, wide = w_one.shape[2:]
        n_steps, rows = inputs.shape[2:4]
        bf, f32 = jnp.bfloat16, jnp.float32
        out_one, out_two = pl.pallas_call(
            lambda *refs: run_kernel(n_dev, n_inner, *refs),
            out_shape=(jax.ShapeDtypeStruct((n_layers, feat, wide), f32), jax.ShapeDtypeStruct((n_layers, wide, feat), f32)),
            in_specs=[pl.BlockSpec(memory_space=pltpu.SMEM)] + [pl.BlockSpec(memory_space=pltpu.HBM)] * 4,
            out_specs=(pl.BlockSpec(memory_space=pl.ANY),) * 2,
            scratch_shapes=[
                pltpu.VMEM((n_steps, rows, feat), bf), pltpu.VMEM((n_steps, rows, feat), bf),
                pltpu.VMEM((n_layers, feat, wide), f32), pltpu.VMEM((n_layers, wide, feat), f32),
                pltpu.VMEM((2, n_layers, feat, wide), bf), pltpu.VMEM((2, n_layers, wide, feat), bf),
                pltpu.VMEM((n_steps, n_layers, feat, wide), bf), pltpu.VMEM((n_steps, n_layers, wide, feat), bf),
                pltpu.VMEM((n_steps, n_layers, feat, wide), bf), pltpu.VMEM((n_steps, n_layers, wide, feat), bf),
                pltpu.VMEM((n_layers, rows, feat), bf), pltpu.VMEM((n_layers, rows, wide), bf),
                pltpu.VMEM((n_layers, rows, wide), f32), pltpu.VMEM((n_layers, rows, feat), f32),
                pltpu.VMEM((n_layers, rows, feat), f32),
                pltpu.SemaphoreType.DMA((2 * n_layers + 2,)), pltpu.SemaphoreType.DMA((2, 2 * n_layers)),
                pltpu.SemaphoreType.DMA((n_steps, 2 * n_layers)), pltpu.SemaphoreType.DMA((2, 2 * n_layers)),
                pltpu.SemaphoreType.DMA((n_steps, 2 * n_layers)), pltpu.SemaphoreType.REGULAR((len(GATES),)),
            ],
            compiler_params=pltpu.CompilerParams(collective_id=0, has_side_effects=True, vmem_limit_bytes=60 * 1024 * 1024),
            name="gossip_run",
        )(mix_self[0, 0], inputs[0, 0], targets[0, 0], w_one[0, 0], w_two[0, 0])
        return out_one[None, None], out_two[None, None]

    return jax.shard_map(device_run, mesh=mesh, in_specs=(spec,) * 5, out_specs=(spec, spec), check_vma=False)
```
